64 devices in a mesh: dp: 4 (over x, y), tp: 16 (over z, core).
Axes of the slice: x: 2, y: 2, z: 8, core: 2. Of those that a mesh axis runs over, the one named last changes fastest.
The devices are a block of a 4x4x8 slice.
Arguments:
- hidden: bfloat16 [32768, 768], P(('dp', 'tp')), parts along dimension 0
- ln_gain: float32 [768], replicated
- ln_bias: float32 [768], replicated
- out_embed: bfloat16 [51200, 768], P('tp')
- vocab_valid: int32 [51200], P('tp')
- targets: int32 [32768], P(('dp', 'tp')), parts along dimension 0
- loss_mask: int32 [32768], P(('dp', 'tp')), parts along dimension 0
Outputs:
- output 1: float32 [32768], P(('dp', 'tp')), parts along dimension 0
- output 2: float32 [4], P('dp'), parts along dimension 0
- output 3: bfloat16 [32768, 768], P(('dp', 'tp')), parts along dimension 0
- output 4: float32 [204800, 768], P(('dp', 'tp')), parts along dimension 0
- output 5: float32 [3072], P('dp'), parts along dimension 0
- output 6: float32 [3072], P('dp'), parts along dimension 0
There are 4 independent parts. The reference program is written for one: setup_inputs(seed, part) draws one part's arguments, and reference() takes and returns one part's arrays. A program takes and returns all parts, laid end to end along the dimension named above; an argument that names none is the same for every part.
All inputs are finite; a program needn't handle non-finite values.
Results may differ from the reference program's by a relative error of at most 0.001.
Values are sent between devices in bfloat16 or wider.
A program may use at most 768 MiB of HBM per device.

```python
import jax
import jax.numpy as jnp
from jax import lax

MODEL_DIM = 768
VOCAB_REAL = 50257
VOCAB_PAD = 51200
SEQ_LEN = 8192
TOK_BLOCK = 512
BLOCK_COUNT = SEQ_LEN // TOK_BLOCK
SOFT_CAP = 30.0
Z_COEF = 1e-4
LN_EPS = 1e-5


def layer_norm(h_float, ln_gain, ln_bias):
    mean_val = jnp.mean(h_float, axis=-1, keepdims=True)
    centered = h_float - mean_val
    var_val = jnp.mean(centered * centered, axis=-1, keepdims=True)
    return centered * lax.rsqrt(var_val + LN_EPS) * ln_gain + ln_bias


def draw_layout(shared_key, part_key):
    col_idx = jnp.arange(VOCAB_PAD)
    coin_draw = jax.random.randint(shared_key, (VOCAB_PAD,), 0, 8)
    dropped = (col_idx % 2 == 0) & (coin_draw == 0) & (col_idx < VOCAB_REAL - 1)
    vocab_valid = ((col_idx < VOCAB_REAL) & jnp.logical_not(dropped)).astype(jnp.int32)
    key_tgt, key_pre, key_post, key_hole = jax.random.split(part_key, 4)
    raw_tgt = jax.random.randint(key_tgt, (SEQ_LEN,), 0, VOCAB_REAL)
    targets = raw_tgt + 1 - vocab_valid[raw_tgt]
    positions = jnp.arange(SEQ_LEN)
    prefix_len = jax.random.randint(key_pre, (), 0, SEQ_LEN // 4 + 1)
    suffix_len = jax.random.randint(key_post, (), 0, SEQ_LEN // 4 + 1)
    hole_draw = jax.random.randint(key_hole, (SEQ_LEN,), 0, 8)
    keep_tok = (positions >= prefix_len) & (positions < SEQ_LEN - suffix_len) & (hole_draw != 0)
    keep_tok = keep_tok | (positions == SEQ_LEN // 2)
    return vocab_valid, targets.astype(jnp.int32), keep_tok.astype(jnp.int32)


def setup_inputs(seed: int = 0, part: int = 0) -> dict:
    shared_key = jax.random.key(seed)
    part_key = jax.random.fold_in(jax.random.key(seed + 1), part)
    key_gain, key_bias, key_embed, key_valid = jax.random.split(shared_key, 4)
    key_hidden, key_layout = jax.random.split(part_key, 2)
    hidden = 1.5 * jax.random.normal(key_hidden, (SEQ_LEN, MODEL_DIM), jnp.float32)
    ln_gain = 1.0 + 0.3 * jax.random.normal(key_gain, (MODEL_DIM,), jnp.float32)
    ln_bias = 0.3 * jax.random.normal(key_bias, (MODEL_DIM,), jnp.float32)
    out_embed = (3.0 * MODEL_DIM ** -0.5) * jax.random.normal(key_embed, (VOCAB_PAD, MODEL_DIM), jnp.float32)
    vocab_valid, targets, loss_mask = draw_layout(key_valid, key_layout)
    return {"hidden": hidden.astype(jnp.bfloat16), "ln_gain": ln_gain, "ln_bias": ln_bias, "out_embed": out_embed.astype(jnp.bfloat16), "vocab_valid": vocab_valid, "targets": targets, "loss_mask": loss_mask}


def reference(hidden, ln_gain, ln_bias, out_embed, vocab_valid, targets, loss_mask):
    normed, ln_back = jax.vjp(layer_norm, hidden.astype(jnp.float32), ln_gain, ln_bias)
    x_all = normed.astype(jnp.bfloat16)
    mask_f = loss_mask.astype(jnp.float32)
    tok_count = jnp.sum(mask_f)
    col_ok = (vocab_valid != 0)[None, :]
    col_ids = jnp.arange(VOCAB_PAD)[None, :]

    def block_step(embed_grad, blk_data):
        x_blk, tgt_blk, mask_blk = blk_data
        logits = jnp.dot(x_blk, out_embed.T, preferred_element_type=jnp.float32)
        tanh_val = jnp.tanh(logits / SOFT_CAP)
        capped = SOFT_CAP * tanh_val
        masked = jnp.where(col_ok, capped, -SOFT_CAP)
        row_max = jnp.max(masked, axis=1, keepdims=True)
        exp_vals = jnp.where(col_ok, jnp.exp(masked - row_max), 0.0)
        sum_exp = jnp.sum(exp_vals, axis=1, keepdims=True)
        lse = row_max[:, 0] + jnp.log(sum_exp[:, 0])
        is_target = tgt_blk[:, None] == col_ids
        tgt_logit = jnp.sum(jnp.where(is_target, capped, 0.0), axis=1)
        tok_loss = (lse - tgt_logit + Z_COEF * lse * lse) * mask_blk
        tok_coef = mask_blk / tok_count
        d_capped = ((1.0 + 2.0 * Z_COEF * lse) * tok_coef)[:, None] * (exp_vals / sum_exp) - jnp.where(is_target, tok_coef[:, None], 0.0)
        d_logits = (d_capped * (1.0 - tanh_val * tanh_val)).astype(jnp.bfloat16)
        new_grad = embed_grad + jnp.dot(d_logits.T, x_blk, preferred_element_type=jnp.float32)
        d_normed = jnp.dot(d_logits, out_embed, preferred_element_type=jnp.float32)
        return new_grad, (tok_loss, d_normed)

    init_grad = jnp.zeros((VOCAB_PAD, MODEL_DIM), jnp.float32)
    blk_inputs = (x_all.reshape(BLOCK_COUNT, TOK_BLOCK, MODEL_DIM), targets.reshape(BLOCK_COUNT, TOK_BLOCK), mask_f.reshape(BLOCK_COUNT, TOK_BLOCK))
    d_embed, (tok_loss, d_normed) = lax.scan(block_step, init_grad, blk_inputs)
    tok_loss = tok_loss.reshape(SEQ_LEN)
    d_normed = d_normed.reshape(SEQ_LEN, MODEL_DIM)
    mean_loss = jnp.sum(tok_loss) / tok_count
    d_hidden, d_gain, d_bias = ln_back(d_normed)
    return tok_loss, mean_loss.reshape(1), d_hidden.astype(jnp.bfloat16), d_embed, d_gain, d_bias
```

```python
import functools

import jax
import jax.numpy as jnp
from jax import lax
from jax.experimental import pallas as pl
from jax.experimental.pallas import tpu as pltpu
from jax.sharding import PartitionSpec as P

SOFT_CAP = 30.0
Z_COEF = 1e-4
LN_EPS = 1e-5
CAP_LOG2E = SOFT_CAP * 1.4426950408889634
NEG = -1e4
MESH = pl.DeviceIdType.MESH
F32 = jnp.float32
BF16 = jnp.bfloat16
LANES = 128
RS_SLOTS = 4


def pick_chunk(vocab_loc):
    for cand in (640, 512, 384, 320, 256, 128, 64, 32, 16):
        if vocab_loc % cand == 0:
            return cand
    raise ValueError("vocab shard")


def kernel(nch, h_ref, gain_ref, bias_ref, e_hbm, val_ref, aux_ref,
           tok_ref, gb_ref, dh_ref, de_out, t_hbm,
           e_v, et_v, xp, de_v, negb, xh_v, rstd_v, zb, tb, dzb, rsr, sbuf, p_own, p_par, p_rcv, dxn,
           auxo, auxq, st_o, st_q, st_r, cf_o, cf_q, cur, acc_g, acc_b, gb_s, gb_r, lossp,
           esem, ag_s, ag_r, dd_s, dd_r, ax_s, ax_r, aq_s, aq_r, ss_s, ss_r, cs_s, cs_r, gs_s, gs_r,
           tsem, rs_s, rs_r, pd_s, pd_r, osem, credit):
    toks, dim = h_ref.shape
    th = toks // 2
    pair = 2 * th
    nj = pair // LANES
    njh = nj // 2
    vloc = e_v.shape[0]
    vc = zb.shape[0]
    nv = vloc // vc
    nunit = 2 * nch
    last = nunit - 1
    sub = 64 if vc % 64 == 0 else 16
    tslots = tb.shape[0]

    me = lax.axis_index("tp")
    chip = me // 2
    core = me % 2
    dirn = 2 * core - 1

    def dev(chip_idx, core_idx):
        return {"tp": lax.rem(chip_idx + 4 * nch, nch) * 2 + core_idx}

    nxt = dev(chip + dirn, core)
    prv = dev(chip - dirn, core)
    par = dev(chip, 1 - core)

    e_copy = pltpu.make_async_copy(e_hbm, e_v, esem)
    e_copy.start()

    barrier = pltpu.get_barrier_semaphore()
    for peer in (nxt, prv, par):
        pl.semaphore_signal(barrier, inc=1, device_id=peer, device_id_type=MESH)

    def remote(src, dst, ssem, rsem, device):
        return pltpu.make_async_remote_copy(src_ref=src, dst_ref=dst, send_sem=ssem, recv_sem=rsem, device_id=device, device_id_type=MESH)

    def ag_ring(s, h):
        return remote(xp.at[s, h, pl.ds(0, th)], xp.at[s + 1, h, pl.ds(0, th)], ag_s.at[s, h], ag_r.at[s + 1, h], nxt)

    def ag_recv(s, h):
        return remote(xp.at[s, h, pl.ds(0, th)], xp.at[s, h, pl.ds(0, th)], ag_s.at[s, h], ag_r.at[s, h], nxt)

    def ag_d2d(s, h):
        return remote(xp.at[s, h, pl.ds(0, th)], xp.at[s, h, pl.ds(th, th)], dd_s.at[s, h], dd_r.at[s, h], par)

    def aux_ring(s):
        return remote(auxo.at[s], auxo.at[s + 1], ax_s.at[s], ax_r.at[s + 1], nxt)

    def aux_recv(s):
        return remote(auxo.at[s], auxo.at[s], ax_s.at[s], ax_r.at[s], nxt)

    def aux_d2d(s):
        return remote(auxo.at[s], auxq.at[s], aq_s.at[s], aq_r.at[s], par)

    gain = gain_ref[...]
    bias = bias_ref[...]

    def ln_rows(r0):
        hf = h_ref[pl.ds(r0, 64), :].astype(F32)
        mean = jnp.mean(hf, axis=1, keepdims=True)
        cent = hf - mean
        var = jnp.mean(cent * cent, axis=1, keepdims=True)
        rstd = lax.rsqrt(var + LN_EPS)
        xh = cent * rstd
        return xh, rstd

    auxo[0] = aux_ref[...]
    for h in range(2):
        for r in range(0, th, 64):
            xh, rstd = ln_rows(h * th + r)
            xh_v[h * th + r:h * th + r + 64, :] = xh
            rstd_v[h * th + r:h * th + r + 64, :] = jnp.broadcast_to(rstd, (64, LANES))
            xp[0, h, r:r + 64, :] = (xh * gain + bias).astype(BF16)
        if h == 0:
            pl.semaphore_wait(barrier, 3)
            aux_ring(0).start()
            aux_d2d(0).start()
        ag_ring(0, h).start()
        ag_d2d(0, h).start()

    def neg_rows(b, _):
        row = jnp.where(val_ref[pl.ds(b, 1), :] != 0, 0.0, NEG).astype(F32)
        blk = jnp.broadcast_to(row, (LANES, LANES))
        negb[pl.ds(pl.multiple_of(b * LANES, LANES), LANES), :] = blk.T
        return 0

    lax.fori_loop(0, vloc // LANES, neg_rows, 0)
    e_copy.wait()

    rio8 = lax.broadcasted_iota(jnp.int32, (8, LANES), 0).astype(F32)
    vbase = (me * vloc).astype(F32)

    def tgt_rows(s, h):
        t_own = auxo[s]
        t_par = auxq[s]
        rows = []
        for tile in (t_own, t_par):
            for j in range(njh):
                rows.append(jnp.where(h == 0, tile[j:j + 1, :], tile[njh + j:njh + j + 1, :]))
        return rows

    def mm(s, h, i):
        r0 = pl.multiple_of(i * vc, vc)
        return lax.dot_general(e_v[pl.ds(r0, vc), :], xp[s, h], (((1,), (1,)), ((), ())), preferred_element_type=F32)

    def ew(s, h, i, slot, carry):
        sums, tsel = list(carry[0]), list(carry[1])
        r0 = pl.multiple_of(i * vc, vc)
        base = vbase + (i * vc).astype(F32)
        rows = tgt_rows(s, h)
        tgb = [jnp.broadcast_to(rows[j] - base, (8, LANES)) - rio8 for j in range(nj)]
        for r in range(0, vc, sub):
            neg = negb[pl.ds(r0 + r, sub), :]
            for j in range(nj):
                cols = slice(j * LANES, (j + 1) * LANES)
                t = jnp.tanh(zb[r:r + sub, cols] * (1.0 / SOFT_CAP)) + neg
                tb[slot, r:r + sub, cols] = t
                sums[j] = sums[j] + jnp.exp2(t * CAP_LOG2E).reshape(sub // 8, 8, LANES).sum(0)
                for g in range(sub // 8):
                    hit = tgb[j] == float(r + g * 8)
                    tsel[j] = jnp.where(hit, t[g * 8:g * 8 + 8], tsel[j])
        return tuple(sums), tuple(tsel)

    zeros8 = jnp.zeros((8, LANES), F32)
    zcarry = ((zeros8,) * nj, (zeros8,) * nj)

    def t_out(s, h, i, slot):
        return pltpu.make_async_copy(tb.at[slot], t_hbm.at[s, h, pl.ds(pl.multiple_of(i * vc, vc), vc)], tsem.at[slot])

    def flush(s, h, carry):
        for which in range(2):
            dst = st_o if which == 0 else st_q
            for hh in range(2):
                @pl.when(h == hh)
                def _():
                    for j in range(njh):
                        jj = which * njh + j
                        dst[s, hh * njh + j, :] = jnp.sum(carry[0][jj], axis=0)
                        dst[s, 2 * njh + hh * njh + j, :] = jnp.sum(carry[1][jj], axis=0)

        @pl.when(h == 1)
        def _():
            @pl.when(s == 0)
            def _():
                st_r[0] = st_o[0]

            @pl.when(s > 0)
            def _():
                remote(st_o.at[s], st_r.at[s], ss_s.at[s], ss_r.at[s], dev(chip - s * dirn, core)).start()
            remote(st_q.at[s], st_r.at[nch + s], ss_s.at[nch + s], ss_r.at[nch + s], dev(chip + s * dirn, 1 - core)).start()

    def fwd_step(q, i, carry):
        s, h = q // 2, q % 2
        n = q * nv + i
        m = n - 1
        slot = lax.rem(m + tslots, tslots)
        qm = jnp.maximum(m, 0) // nv
        im = jnp.maximum(m, 0) - qm * nv
        sm, hm = qm // 2, qm % 2

        @pl.when(m >= tslots)
        def _():
            t_out(sm, hm, im, slot).wait()
        carry = ew(sm, hm, im, slot, carry)
        zb[...] = mm(s, h, i)

        @pl.when(m >= 0)
        def _():
            t_out(sm, hm, im, slot).start()
        return carry, (sm, hm)

    def fwd_unit(q, carry):
        q1 = q + 1
        s1, h1 = q1 // 2, q1 % 2

        @pl.when((q1 >= 2) & (q1 < nunit))
        def _():
            ag_recv(s1, h1).wait_recv()

            @pl.when(s1 < nch - 1)
            def _():
                ag_ring(s1, h1).start()
            ag_d2d(s1, h1).start()

            @pl.when(h1 == 0)
            def _():
                aux_recv(s1).wait_recv()

                @pl.when(s1 < nch - 1)
                def _():
                    aux_ring(s1).start()
                aux_d2d(s1).start()

        s, h = q // 2, q % 2
        remote(xp.at[s, h, pl.ds(th, th)], xp.at[s, h, pl.ds(th, th)], dd_s.at[s, h], dd_r.at[s, h], par).wait_recv()

        @pl.when(h == 0)
        def _():
            remote(auxq.at[s], auxq.at[s], aq_s.at[s], aq_r.at[s], par).wait_recv()
        carry, (sm, hm) = fwd_step(q, jnp.int32(0), carry)

        @pl.when(q > 0)
        def _():
            flush(sm, hm, carry)
        return lax.fori_loop(1, nv, lambda i, c: fwd_step(q, i, c)[0], zcarry)

    carry = lax.fori_loop(0, nunit, fwd_unit, zcarry)
    m_last = nunit * nv - 1
    slot_l = m_last % tslots
    s_l, h_l, i_l = jnp.int32(nch - 1), jnp.int32(1), jnp.int32(nv - 1)
    t_out(s_l, h_l, i_l, slot_l).wait()
    carry = ew(s_l, h_l, i_l, slot_l, carry)
    t_out(s_l, h_l, i_l, slot_l).start()
    flush(s_l, h_l, carry)

    def tr_rows(b, _):
        v0 = pl.multiple_of(b * LANES, LANES)
        et_v[:, pl.ds(v0, LANES)] = e_v[pl.ds(v0, LANES), :].T
        return 0

    lax.fori_loop(0, vloc // LANES, tr_rows, 0)

    def zero_rows(b, _):
        de_v[pl.ds(pl.multiple_of(b * LANES, LANES), LANES), :] = jnp.zeros((LANES, dim), F32)
        return 0

    lax.fori_loop(0, vloc // LANES, zero_rows, 0)

    for m in range(m_last - tslots + 1, m_last + 1):
        qm = m // nv
        t_out(qm // 2, qm % 2, m % nv, m % tslots).wait()

    def a_of(s):
        return lax.rem(s + 1, nch)

    def t_in(n):
        q = n // nv
        i = n - q * nv
        slot = lax.rem(n, tslots)
        s, h = q // 2, q % 2
        return pltpu.make_async_copy(t_hbm.at[a_of(s), h, pl.ds(pl.multiple_of(i * vc, vc), vc)], tb.at[slot], tsem.at[slot])

    for n in range(tslots - 1):
        t_in(jnp.int32(n)).start()

    for s in range(1, nch):
        remote(st_o.at[s], st_r.at[s], ss_s.at[s], ss_r.at[s], par).wait_recv()
    for s in range(nch):
        remote(st_q.at[s], st_r.at[nch + s], ss_s.at[nch + s], ss_r.at[nch + s], par).wait_recv()
    half = 2 * njh
    tot = st_r[0]
    for s in range(1, 2 * nch):
        tot = tot + st_r[s]
    cnt = auxo[0, half:, :]
    for s in range(nch):
        if s > 0:
            cnt = cnt + auxo[s, half:, :]
        cnt = cnt + auxq[s, half:, :]
    n_tok = jnp.sum(jnp.sum(cnt, axis=1, keepdims=True), axis=0, keepdims=True)
    inv_n = 1.0 / n_tok
    sumexp = tot[0:half]
    lse = jnp.log(sumexp)
    mask = auxo[0, half:, :]
    tok_loss = (lse - SOFT_CAP * tot[half:] + Z_COEF * lse * lse) * mask
    tok_ref[...] = tok_loss
    lossp[...] = jnp.sum(tok_loss, axis=0, keepdims=True)
    c_tgt = mask * inv_n
    cf_o[0, 0:half, :] = (1.0 + 2.0 * Z_COEF * lse) * c_tgt / sumexp
    cf_o[0, half:, :] = c_tgt

    def cf_send_o(s):
        return remote(cf_o.at[0], cf_o.at[s], cs_s.at[s], cs_r.at[s], dev(chip + s * dirn, core))

    def cf_send_q(s):
        return remote(cf_o.at[0], cf_q.at[s], cs_s.at[nch + s], cs_r.at[nch + s], dev(chip + s * dirn, 1 - core))

    for s in range(1, nch):
        cf_send_o(s).start()
        cf_send_q(s).start()
    cf_send_q(0).start()

    def prep(q):
        s, h = q // 2, q % 2
        a = a_of(s)

        @pl.when(h == 0)
        def _():
            @pl.when(a > 0)
            def _():
                remote(cf_o.at[a], cf_o.at[a], cs_s.at[a], cs_r.at[a], par).wait_recv()
            remote(cf_q.at[a], cf_q.at[a], cs_s.at[nch + a], cs_r.at[nch + a], par).wait_recv()
        rows = tgt_rows(a, h)
        for j in range(nj):
            cur[8 + j:9 + j, :] = rows[j]
        for w, tile in enumerate((cf_o[a], cf_q[a])):
            for j in range(njh):
                for part in range(2):
                    o = part * half
                    cur[part * nj + w * njh + j:part * nj + w * njh + j + 1, :] = jnp.where(
                        h == 0, tile[o + j:o + j + 1, :], tile[o + njh + j:o + njh + j + 1, :])

    def dz_chunk(q, i, slot):
        r0 = pl.multiple_of(i * vc, vc)
        base = vbase + (i * vc).astype(F32)
        dslot = q % 2
        c1 = [jnp.broadcast_to(cur[j:j + 1, :], (8, LANES)) for j in range(nj)]
        ct = [jnp.broadcast_to(cur[nj + j:nj + j + 1, :], (8, LANES)) for j in range(nj)]
        tgb = [jnp.broadcast_to(cur[8 + j:9 + j, :] - base, (8, LANES)) - rio8 for j in range(nj)]
        for r in range(0, vc, 16):
            for j in range(nj):
                cols = slice(j * LANES, (j + 1) * LANES)
                parts = []
                for g in range(2):
                    t = tb[slot, r + 8 * g:r + 8 * g + 8, cols]
                    d = c1[j] * jnp.exp2(t * CAP_LOG2E)
                    d = jnp.where(tgb[j] == float(r + 8 * g), d - ct[j], d)
                    parts.append(d * (1.0 - t * t))
                dzb[dslot, pl.ds(r0 + r, 16), cols] = jnp.concatenate(parts, axis=0).astype(BF16)

    def de_chunk(q, i):
        s, h = q // 2, q % 2
        r0 = pl.multiple_of(i * vc, vc)
        acc = jnp.dot(dzb[q % 2, pl.ds(r0, vc), :], xp[a_of(s), h], preferred_element_type=F32)
        de_v[pl.ds(r0, vc), :] = de_v[pl.ds(r0, vc), :] + acc

    def stage_a(q, with_de):
        def step(i, _):
            n = q * nv + i
            slot = lax.rem(n, tslots)
            t_in(n).wait()

            @pl.when(n + tslots - 1 < nunit * nv)
            def _():
                t_in(n + tslots - 1).start()
            dz_chunk(q, i, slot)
            if with_de:
                de_chunk(q - 1, i)
            return 0
        lax.fori_loop(0, nv, step, 0)

    def p_send(q):
        return remote(p_par, p_rcv.at[q % 2], pd_s, pd_r.at[q % 2], par)

    def stage_c(q, first):
        if not first:
            p_send(q).wait_send()
        out = jnp.dot(et_v[...], dzb[q % 2], preferred_element_type=F32)
        p_par[...] = out[:, th:]
        p_own[...] = out[:, :th]
        p_send(q).start()

    def rs_send(q):
        return remote(sbuf.at[q % 2], rsr.at[lax.rem(q + 2, RS_SLOTS)], rs_s.at[q % 2], rs_r.at[lax.rem(q + 2, RS_SLOTS)], nxt)

    def rs_wait(q):
        slot = lax.rem(q, RS_SLOTS)
        remote(rsr.at[slot], rsr.at[slot], rs_s.at[q % 2], rs_r.at[slot], nxt).wait_recv()

    def p_wait(q):
        remote(p_rcv.at[q % 2], p_rcv.at[q % 2], pd_s, pd_r.at[q % 2], par).wait_recv()

    rb = 64 if dim % 64 == 0 else 16

    def stage_b(q):
        p_wait(q)

        @pl.when(q >= 2)
        def _():
            rs_wait(q)
            rs_send(q - 2).wait_send()

        @pl.when(q >= RS_SLOTS)
        def _():
            pl.semaphore_wait(credit, 1)
        slot = lax.rem(q, RS_SLOTS)

        @pl.when(q < 2)
        def _():
            def add2(b, _):
                rows = pl.ds(pl.multiple_of(b * rb, rb), rb)
                sbuf[q % 2, rows, :] = p_own[rows, :] + p_rcv[q % 2, rows, :]
                return 0
            lax.fori_loop(0, dim // rb, add2, 0)

        @pl.when(q >= 2)
        def _():
            def add3(b, _):
                rows = pl.ds(pl.multiple_of(b * rb, rb), rb)
                sbuf[q % 2, rows, :] = p_own[rows, :] + p_rcv[q % 2, rows, :] + rsr[slot, rows, :]
                return 0
            lax.fori_loop(0, dim // rb, add3, 0)

            @pl.when(q < nunit - RS_SLOTS)
            def _():
                pl.semaphore_signal(credit, inc=1, device_id=prv, device_id_type=MESH)
        rs_send(q).start()

    acc_g[...] = jnp.zeros_like(acc_g)
    acc_b[...] = jnp.zeros_like(acc_b)

    def final_half(h):
        q = jnp.int32(nunit - 2 + h)
        p_wait(q)
        rs_wait(q)
        slot = lax.rem(q, RS_SLOTS)
        for b in range(dim // LANES):
            rows = slice(b * LANES, (b + 1) * LANES)
            for c in range(th // LANES):
                cols = slice(c * LANES, (c + 1) * LANES)
                blk = p_own[rows, cols] + p_rcv[q % 2, rows, cols] + rsr[slot, rows, cols]
                dxn[cols, rows] = blk.T
        for r in range(0, th, 32):
            o = h * th + r
            dx = dxn[r:r + 32, :]
            xh = xh_v[o:o + 32, :]
            rstd = rstd_v[o:o + 32, 0:1]
            acc_g[...] += (dx * xh).reshape(4, 8, dim).sum(0)
            acc_b[...] += dx.reshape(4, 8, dim).sum(0)
            dxh = dx * gain
            m1 = jnp.mean(dxh, axis=1, keepdims=True)
            m2 = jnp.mean(dxh * xh, axis=1, keepdims=True)
            dh_ref[o:o + 32, :] = (rstd * (dxh - m1 - xh * m2)).astype(BF16)

    prep(jnp.int32(0))
    stage_a(jnp.int32(0), False)
    stage_c(jnp.int32(0), True)

    def bwd_unit(q, _):
        prep(q)
        stage_a(q, True)
        stage_b(q - 1)
        stage_c(q, False)
        return 0

    lax.fori_loop(1, nunit - 1, bwd_unit, 0)
    q_l = jnp.int32(last)
    prep(q_l)
    stage_a(q_l, True)
    final_half(0)
    stage_c(q_l, False)

    def de_store(i):
        rows = pl.ds(pl.multiple_of(i * vc, vc), vc)
        return pltpu.make_async_copy(de_v.at[rows], de_out.at[rows], osem.at[i])

    def last_de(i, _):
        de_chunk(q_l, i)
        de_store(i).start()
        return 0

    lax.fori_loop(0, nv, last_de, 0)
    final_half(1)

    ng = dim // LANES
    dg = jnp.sum(acc_g[...], axis=0, keepdims=True)
    db = jnp.sum(acc_b[...], axis=0, keepdims=True)
    gb_s[...] = jnp.zeros_like(gb_s)
    for j in range(ng):
        cols = slice(j * LANES, (j + 1) * LANES)
        gb_s[j:j + 1, :] = dg[:, cols]
        gb_s[ng + j:ng + j + 1, :] = db[:, cols]
    gb_s[2 * ng:2 * ng + 1, :] = lossp[...]

    def gb_send(o):
        return remote(gb_s, gb_r.at[me], gs_s.at[o], gs_r.at[me], {"tp": lax.rem(me + o, 2 * nch)})

    for o in range(1, 2 * nch):
        gb_send(o).start()
    gb_r[me] = gb_s[...]
    for o in range(1, 2 * nch):
        src = lax.rem(me + o, 2 * nch)
        remote(gb_s, gb_r.at[src], gs_s.at[o], gs_r.at[src], par).wait_recv()
    total = gb_r[0]
    for o in range(1, 2 * nch):
        total = total + gb_r[o]
    gb_ref[...] = total
    loss = jnp.sum(total[2 * ng:2 * ng + 1, :], axis=1, keepdims=True) * inv_n
    gb_ref[2 * ng:2 * ng + 1, :] = jnp.broadcast_to(loss, (1, LANES))

    for s in range(nch):
        for h in range(2):
            if s < nch - 1:
                ag_ring(s, h).wait_send()
            ag_d2d(s, h).wait_send()
        if s < nch - 1:
            aux_ring(s).wait_send()
        aux_d2d(s).wait_send()
        if s > 0:
            remote(st_o.at[s], st_r.at[s], ss_s.at[s], ss_r.at[s], par).wait_send()
            cf_send_o(s).wait_send()
        remote(st_q.at[s], st_r.at[nch + s], ss_s.at[nch + s], ss_r.at[nch + s], par).wait_send()
        cf_send_q(s).wait_send()
    for o in range(1, 2 * nch):
        gb_send(o).wait_send()
    p_send(q_l).wait_send()
    rs_send(jnp.int32(nunit - 4)).wait_send()
    rs_send(jnp.int32(nunit - 3)).wait_send()
    for i in range(nv):
        de_store(i).wait()


def solution(mesh):
    ntp = mesh.shape["tp"]
    nch = ntp // 2

    def group_step(hidden, ln_gain, ln_bias, out_embed, vocab_valid, targets, loss_mask):
        toks, dim = hidden.shape
        vloc = out_embed.shape[0]
        th = toks // 2
        pair = 2 * th
        vc = pick_chunk(vloc)
        nv = vloc // vc
        rows = toks // LANES
        aux = jnp.concatenate([targets.reshape(rows, LANES), loss_mask.reshape(rows, LANES)], axis=0).astype(F32)
        val = vocab_valid.reshape(vloc // LANES, LANES)
        ng = dim // LANES
        gbr = -(-(2 * ng + 1) // 8) * 8
        vm = pl.BlockSpec(memory_space=pltpu.VMEM)
        hb = pl.BlockSpec(memory_space=pl.ANY)
        sds = jax.ShapeDtypeStruct
        dma = pltpu.SemaphoreType.DMA
        V = pltpu.VMEM
        outs = pl.pallas_call(
            functools.partial(kernel, nch),
            name="fused_loss",
            out_shape=(sds((rows, LANES), F32), sds((gbr, LANES), F32), sds((toks, dim), BF16), sds((vloc, dim), F32), sds((nch, 2, vloc, pair), F32)),
            in_specs=[vm, vm, vm, hb, vm, vm],
            out_specs=(vm, vm, vm, hb, hb),
            scratch_shapes=[
                V((vloc, dim), BF16), V((dim, vloc), BF16), V((nch, 2, pair, dim), BF16), V((vloc, dim), F32),
                V((vloc, LANES), F32), V((toks, dim), F32), V((toks, LANES), F32), V((vc, pair), F32), V((3, vc, pair), F32),
                V((2, vloc, pair), BF16), V((RS_SLOTS, dim, th), F32), V((2, dim, th), F32), V((dim, th), F32), V((dim, th), F32),
                V((2, dim, th), F32), V((th, dim), F32),
                V((nch, 8, LANES), F32), V((nch, 8, LANES), F32), V((nch, 8, LANES), F32), V((nch, 8, LANES), F32),
                V((2 * nch, 8, LANES), F32), V((nch, 8, LANES), F32), V((nch, 8, LANES), F32), V((16, LANES), F32),
                V((8, dim), F32), V((8, dim), F32), V((gbr, LANES), F32), V((ntp, gbr, LANES), F32), V((1, LANES), F32),
                dma, dma((nch, 2)), dma((nch, 2)), dma((nch, 2)), dma((nch, 2)), dma((nch,)), dma((nch,)), dma((nch,)), dma((nch,)),
                dma((2 * nch,)), dma((2 * nch,)), dma((2 * nch,)), dma((2 * nch,)), dma((ntp,)), dma((ntp,)),
                dma((3,)), dma((2,)), dma((RS_SLOTS,)), dma, dma((2,)), dma((nv,)), pltpu.SemaphoreType.REGULAR,
            ],
            compiler_params=pltpu.CompilerParams(
                collective_id=0, has_side_effects=True, vmem_limit_bytes=66 * 10**6),
            cost_estimate=pl.CostEstimate(flops=6 * vloc * dim * toks * ntp, bytes_accessed=8 * vloc * toks * ntp, transcendentals=0),
        )(hidden, ln_gain.reshape(1, dim), ln_bias.reshape(1, dim), out_embed, val, aux)
        tok, gb, dh, de, _ = outs
        d_gain = gb[0:ng].reshape(dim)
        d_bias = gb[ng:2 * ng].reshape(dim)
        return tok.reshape(toks), gb[2 * ng, 0:1], dh, de, d_gain, d_bias

    row_spec = P(("dp", "tp"))
    mat_spec = P(("dp", "tp"), None)
    return jax.shard_map(group_step, mesh=mesh, in_specs=(mat_spec, P(None), P(None), P("tp", None), P("tp"), row_spec, row_spec), out_specs=(row_spec, P("dp"), mat_spec, mat_spec, P("dp"), P("dp")), check_vma=False)
```
